32 devices in a mesh: frames: 8 (over z, y), heads: 4 (over x, core).
Axes of the slice: x: 2, y: 2, z: 4, core: 2. Of those that a mesh axis runs over, the one named last changes fastest.
Arguments:
- tokens: bfloat16 [1024, 4096], P('frames'), may hold values from -6 to 6
- norm_gain: float32 [4096], replicated, may hold values from 0.5 to 1.5
- w_query: bfloat16 [4096, 2048], P(None, 'heads'), may hold values from -0.09375 to 0.09375
- w_key: bfloat16 [4096, 2048], P(None, 'heads'), may hold values from -0.09375 to 0.09375
- w_value: bfloat16 [4096, 2048], P(None, 'heads'), may hold values from -0.09375 to 0.09375
- head_gain: float32 [2048], P('heads'), may hold values from 0.5 to 1.5
- w_out: bfloat16 [2048, 4096], P('heads'), may hold values from -0.125 to 0.125
Outputs:
- mixed: bfloat16 [1024, 4096], P('frames', 'heads')
The draws below stay inside these ranges and needn't reach their ends.
All inputs are finite; a program needn't handle non-finite values.
Results may differ from the reference program's by a relative error of at most 0.015.
Values may be sent and summed in bfloat16 or wider, within the bound.
A program may use at most 128 MiB of HBM per device.

```python
import math
import jax
import jax.numpy as jnp
from jax import lax

D = 4096
HD = 128
TOK_DEV = 128
HEADS = 16
TOKENS = 1024


def levels(own_key, dims, shards, smallest, top_value):
    loudness, own = 1.0, jax.random.fold_in(own_key, 6)
    for dim, shards_of in shards:
        heights = jnp.exp(jax.random.uniform(jax.random.fold_in(own, dim), (shards_of,), jnp.float32, smallest / len(shards), top_value / len(shards)))
        loudness = loudness * jnp.repeat(heights, dims[dim] // shards_of).reshape([-1 if axis == dim else 1 for axis in range(len(dims))])
    return loudness


def centred(key, shape, deviation, limit, cuts=(), held_as=jnp.bfloat16):
    values = deviation * jax.random.normal(key, shape, jnp.float32)
    if cuts:
        values = values * levels(key, shape, cuts, -0.22, 0.18)
    return jnp.clip(values, -limit, limit).astype(held_as)


def setup_inputs(seed: int = 0) -> dict:
    keys = jax.random.split(jax.random.key(seed), 8)
    tokens = centred(keys[0], (TOKENS, D), 1.0, 6.0, ((0, 8),))
    norm_gain = jnp.clip(1.0 + 0.1 * jax.random.normal(keys[1], (D,), jnp.float32), 0.5, 1.5)
    w_query = centred(keys[2], (D, HEADS * HD), D ** -0.5, 0.09375, ((1, 4),))
    w_key = centred(keys[3], (D, HEADS * HD), D ** -0.5, 0.09375, ((1, 4),))
    w_value = centred(keys[4], (D, HEADS * HD), D ** -0.5, 0.09375, ((1, 4),))
    head_gain = jnp.clip(1.0 + 0.1 * jax.random.normal(keys[5], (HEADS * HD,), jnp.float32), 0.5, 1.5)
    w_out = centred(keys[6], (HEADS * HD, D), (HEADS * HD) ** -0.5, 0.125, ((0, 4),))
    return {"tokens": tokens, "norm_gain": norm_gain, "w_query": w_query, "w_key": w_key, "w_value": w_value, "head_gain": head_gain, "w_out": w_out}


epsilon = 1e-06

def reference(tokens, norm_gain, w_query, w_key, w_value, head_gain, w_out):
    widened = tokens.astype(jnp.float32)
    normed = (widened * lax.rsqrt(lax.optimization_barrier(jnp.mean(widened * widened, axis=1, keepdims=True)) + epsilon) * norm_gain[None, :]).astype(jnp.bfloat16)
    query_rows = jnp.dot(normed, w_query, preferred_element_type=jnp.float32).astype(jnp.bfloat16)
    key_rows = jnp.dot(normed, w_key, preferred_element_type=jnp.float32).astype(jnp.bfloat16)
    value_rows = jnp.dot(normed, w_value, preferred_element_type=jnp.float32).astype(jnp.bfloat16)
    block_count = TOKENS // TOK_DEV
    query_blocks = query_rows.astype(jnp.float32).reshape(block_count, TOK_DEV, HEADS, HD)
    key_blocks = key_rows.astype(jnp.float32).reshape(block_count, TOK_DEV, HEADS, HD)
    value_blocks = value_rows.astype(jnp.float32).reshape(block_count, TOK_DEV, HEADS, HD)
    inv_root = 1.0 / math.sqrt(HD)

    def one_block(packed):
        block_index, query_block = packed
        query_pos = block_index * TOK_DEV + jnp.arange(TOK_DEV, dtype=jnp.int32)

        def advance(column, state):
            running_max, running_sum, weighted = state
            key_block = lax.dynamic_index_in_dim(key_blocks, column, 0, keepdims=False)
            value_block = lax.dynamic_index_in_dim(value_blocks, column, 0, keepdims=False)
            scores = jnp.einsum('qhd,khd->hqk', query_block, key_block) * inv_root
            key_pos = column * TOK_DEV + jnp.arange(TOK_DEV, dtype=jnp.int32)
            visible = (key_pos[None, :] <= query_pos[:, None])[None]
            scores = jnp.where(visible, scores, jnp.float32(-1e+30))
            top = jnp.maximum(running_max, lax.optimization_barrier(jnp.max(scores, axis=2)))
            expscores = jnp.where(visible, jnp.exp(scores - top[:, :, None]), jnp.float32(0.0))
            shrink = jnp.exp(running_max - top)
            running_sum = running_sum * shrink + lax.optimization_barrier(jnp.sum(expscores, axis=2))
            weighted = weighted * shrink[:, :, None] + jnp.einsum('hqk,khd->hqd', expscores, value_block)
            return (top, running_sum, weighted)
        initial = (jnp.full((HEADS, TOK_DEV), -1e+30, jnp.float32), jnp.zeros((HEADS, TOK_DEV), jnp.float32), jnp.zeros((HEADS, TOK_DEV, HD), jnp.float32))
        running_max, running_sum, weighted = lax.fori_loop(jnp.int32(0), block_index + 1, advance, initial)
        attended = weighted / running_sum[:, :, None]
        scaled = attended * lax.rsqrt(lax.optimization_barrier(jnp.mean(attended * attended, axis=2, keepdims=True)) + epsilon) * head_gain.reshape(HEADS, 1, HD)
        return jnp.transpose(scaled, (1, 0, 2)).reshape(TOK_DEV, HEADS * HD).astype(jnp.bfloat16)
    headed = lax.map(one_block, (jnp.arange(block_count, dtype=jnp.int32), query_blocks))
    headed = headed.reshape(TOKENS, HEADS * HD)
    return jnp.dot(headed, w_out, preferred_element_type=jnp.float32).astype(jnp.bfloat16)
```

```python
import functools
import math

import jax
import jax.numpy as jnp
from jax import lax
from jax.experimental import pallas as pl
from jax.experimental.pallas import tpu as pltpu
from jax.sharding import PartitionSpec as P

HD = 128
EPS = 1e-06
MESH = pl.DeviceIdType.MESH


def fused_kernel(
    n, nh,
    tokens_hbm, norm_gain_ref, wq_hbm, wk_hbm, wv_hbm, head_gain_ref, wo_hbm,
    out_ref,
    tok, normed, wkv, wq, wo, kvout, qout, kv, q, oout, headed, s1, r1, s2, r2, acc,
    tok_sem, w_sem, wo_sem,
    kvs_sem, qs_sem, fw_sem, kvr_sem, qr_sem, os_sem, or_sem,
    s1_sem, r1_sem, s2_sem, r2_sem,
):
    heads = kvout.shape[0]
    rows = tok.shape[0]
    group = n // heads
    half = max(heads // 2, 1)
    me = lax.axis_index("frames")
    lane = lax.axis_index("heads")
    level, member = lax.div(me, group), lax.rem(me, group)
    core, pair = lax.rem(lane, 2), lax.div(lane, 2)
    pairs = nh // 2
    lower = level < half

    def head_at(k):
        return jnp.where(lower, heads - 1 - k, k)

    tok_copy = pltpu.make_async_copy(tokens_hbm, tok, tok_sem)
    tok_copy.start()
    loads = []
    per = 2 if heads % 2 == 0 else 1
    for k in range(heads):
        cols = pl.ds(pl.multiple_of(head_at(k) * HD, HD), HD)
        loads.append((
            pltpu.make_async_copy(wk_hbm.at[:, cols], wkv.at[k, :, pl.ds(0, HD)], w_sem.at[k, 0]),
            pltpu.make_async_copy(wv_hbm.at[:, cols], wkv.at[k, :, pl.ds(HD, HD)], w_sem.at[k, 1]),
            pltpu.make_async_copy(
                wq_hbm.at[:, cols], wq.at[k // per, :, pl.ds((k % per) * HD, HD)], w_sem.at[k, 2]
            ),
        ))
    for first in range(0, heads, per):
        for k in range(first, first + per):
            loads[k][0].start()
            loads[k][1].start()
        for k in range(first, first + per):
            loads[k][2].start()
    wo_copy = pltpu.make_async_copy(wo_hbm, wo, wo_sem)
    wo_copy.start()

    barrier = pltpu.get_barrier_semaphore()
    for d in range(1, heads):
        other = lax.rem(level + d, heads) * group + member
        pl.semaphore_signal(barrier, inc=1, device_id={"frames": other}, device_id_type=MESH)
    for d in range(1, group):
        other = level * group + lax.rem(member + d, group)
        pl.semaphore_signal(barrier, inc=1, device_id={"frames": other}, device_id_type=MESH)
    mate = pair * 2 + 1 - core
    pl.semaphore_signal(barrier, inc=1, device_id={"heads": mate}, device_id_type=MESH)
    for d in range(1, pairs):
        other = lax.rem(pair + d, pairs) * 2 + core
        pl.semaphore_signal(barrier, inc=1, device_id={"heads": other}, device_id_type=MESH)

    tok_copy.wait()
    for start in range(0, rows, 32):
        part = pl.ds(start, 32)
        wide = tok[part, :].astype(jnp.float32)
        scale = lax.rsqrt(jnp.mean(wide * wide, axis=1, keepdims=True) + EPS)
        normed[part, :] = (wide * scale * norm_gain_ref[...]).astype(jnp.bfloat16)

    pl.semaphore_wait(barrier, heads - 1 + group - 1 + 1 + pairs - 1)

    def kv_send(k, target):
        return pltpu.make_async_remote_copy(
            src_ref=kvout.at[k], dst_ref=kv.at[me],
            send_sem=kvs_sem.at[k], recv_sem=kvr_sem.at[me],
            device_id={"frames": target}, device_id_type=MESH,
        )

    def q_send(k, target):
        return pltpu.make_async_remote_copy(
            src_ref=qout.at[k], dst_ref=q.at[level],
            send_sem=qs_sem.at[k], recv_sem=qr_sem.at[level],
            device_id={"frames": target}, device_id_type=MESH,
        )

    def forward(source, d):
        target = level * group + lax.rem(member + d, group)
        return pltpu.make_async_remote_copy(
            src_ref=kv.at[source], dst_ref=kv.at[source],
            send_sem=fw_sem.at[lax.div(source, group), d], recv_sem=kvr_sem.at[source],
            device_id={"frames": target}, device_id_type=MESH,
        )

    def kv_arrived(source):
        return pltpu.make_async_remote_copy(
            src_ref=kv.at[source], dst_ref=kv.at[source],
            send_sem=kvs_sem.at[0], recv_sem=kvr_sem.at[source],
            device_id={"frames": me}, device_id_type=MESH,
        )

    def q_arrived(source):
        return pltpu.make_async_remote_copy(
            src_ref=q.at[source], dst_ref=q.at[source],
            send_sem=qs_sem.at[0], recv_sem=qr_sem.at[source],
            device_id={"frames": me}, device_id_type=MESH,
        )

    for first in range(0, heads, per):
        for k in range(first, first + per):
            loads[k][0].wait()
            loads[k][1].wait()
            block = jnp.dot(normed[...], wkv[k], preferred_element_type=jnp.float32)
            block = block.astype(jnp.bfloat16)
            h = head_at(k)

            @pl.when(h != level)
            def _():
                kvout[k] = block
                kv_send(k, h * group + member).start()

            @pl.when(h == level)
            def _():
                kv[me] = block
                for d in range(1, group):
                    forward(me, d).start()

        for k in range(first, first + per):
            loads[k][2].wait()
        block = jnp.dot(normed[...], wq[first // per], preferred_element_type=jnp.float32)
        block = block.astype(jnp.bfloat16)
        for k in range(first, first + per):
            h = head_at(k)
            part = block[:, (k - first) * HD : (k - first + 1) * HD]

            @pl.when(h != level)
            def _():
                qout[k] = part
                q_send(k, h * group + member).start()

            @pl.when(h == level)
            def _():
                q[level] = part

    for d in range(heads):
        src_level = jnp.where(lower, lax.rem(half + d, heads), lax.rem(half - 1 - d + heads, heads))
        source = src_level * group + member

        @pl.when(src_level != level)
        def _():
            kv_arrived(source).wait_recv()
            for e in range(1, group):
                forward(source, e).start()

    def o_send(i):
        return pltpu.make_async_remote_copy(
            src_ref=oout.at[i],
            dst_ref=headed.at[:, pl.ds(pl.multiple_of(level * HD, HD), HD)],
            send_sem=os_sem.at[i], recv_sem=or_sem.at[level],
            device_id={"frames": i * group + member}, device_id_type=MESH,
        )

    inv_root = 1.0 / math.sqrt(HD)
    gain = head_gain_ref[:, pl.ds(pl.multiple_of(level * HD, HD), HD)]
    for i in range(heads):
        for d in range(1, group):
            kv_arrived(i * group + lax.rem(member + d, group)).wait_recv()

        @pl.when(level != i)
        def _():
            q_arrived(i).wait_recv()

        reach = (i + 1) * group
        keys = kv[:reach, :, :HD].reshape(reach * rows, HD)
        values = kv[:reach, :, HD:].reshape(reach * rows, HD)
        scores = lax.dot_general(
            q[i], keys, (((1,), (1,)), ((), ())), preferred_element_type=jnp.float32
        ) * inv_root
        query_pos = (i * group + member) * rows + lax.broadcasted_iota(jnp.int32, scores.shape, 0)
        key_pos = lax.broadcasted_iota(jnp.int32, scores.shape, 1)
        scores = jnp.where(key_pos <= query_pos, scores, jnp.float32(-1e30))
        top = jnp.max(scores, axis=1, keepdims=True)
        weights = jnp.exp(scores - top)
        total = jnp.sum(weights, axis=1, keepdims=True)
        attended = jnp.dot(
            weights.astype(jnp.bfloat16), values, preferred_element_type=jnp.float32
        ) / total
        scale = lax.rsqrt(jnp.mean(attended * attended, axis=1, keepdims=True) + EPS)
        result = (attended * scale * gain).astype(jnp.bfloat16)

        @pl.when(level != i)
        def _():
            oout[i] = result
            o_send(i).start()

        @pl.when(level == i)
        def _():
            headed[:, pl.ds(pl.multiple_of(level * HD, HD), HD)] = result

    wo_copy.wait()
    for h in range(heads):
        @pl.when(level != h)
        def _():
            here = headed.at[:, pl.ds(h * HD, HD)]
            pltpu.make_async_remote_copy(
                src_ref=here, dst_ref=here, send_sem=os_sem.at[0], recv_sem=or_sem.at[h],
                device_id={"frames": me}, device_id_type=MESH,
            ).wait_recv()

    cw = out_ref.shape[1]
    subs, sw = s1.shape[1], s1.shape[3]
    heads_in = headed[...]

    def partial_at(d, side, s):
        to = lax.rem(pair + d, pairs) * 2 + side
        cols = pl.ds(pl.multiple_of(to * cw + s * sw, sw), sw)
        return jnp.dot(heads_in, wo[:, cols], preferred_element_type=jnp.float32)

    def mate_send(d, s):
        return pltpu.make_async_remote_copy(
            src_ref=s1.at[d, s], dst_ref=r1.at[d, s],
            send_sem=s1_sem.at[d, s], recv_sem=r1_sem.at[d, s],
            device_id={"heads": mate}, device_id_type=MESH,
        )

    def pair_send(d, s):
        return pltpu.make_async_remote_copy(
            src_ref=s2.at[d - 1, s], dst_ref=r2.at[d - 1, s],
            send_sem=s2_sem.at[d - 1, s], recv_sem=r2_sem.at[d - 1, s],
            device_id={"heads": lax.rem(pair + d, pairs) * 2 + core}, device_id_type=MESH,
        )

    order = [(d % pairs, s) for d in range(1, pairs + 1) for s in range(subs)]
    for d, s in order:
        s1[d, s] = partial_at(d, 1 - core, s).astype(jnp.bfloat16)
        mate_send(d, s).start()
    for d, s in order:
        own = partial_at(d, core, s)
        mate_send(d, s).wait_recv()
        own = own + r1[d, s].astype(jnp.float32)
        if d:
            s2[d - 1, s] = own.astype(jnp.bfloat16)
            pair_send(d, s).start()
        else:
            acc[s] = own
    for s in range(subs):
        whole = acc[s]
        for d in range(1, pairs):
            pair_send(d, s).wait_recv()
            whole = whole + r2[d - 1, s].astype(jnp.float32)
        out_ref[:, s * sw : (s + 1) * sw] = whole.astype(jnp.bfloat16)

    for d, s in order:
        mate_send(d, s).wait_send()
        if d:
            pair_send(d, s).wait_send()
    for i in range(heads):
        @pl.when(level != i)
        def _():
            o_send(i).wait_send()

        for d in range(1, group):
            forward(i * group + member, d).wait_send()
    for k in range(heads):
        @pl.when(head_at(k) != level)
        def _():
            kv_send(k, head_at(k) * group + member).wait_send()
            q_send(k, head_at(k) * group + member).wait_send()


def solution(mesh):
    n, nh = mesh.shape["frames"], mesh.shape["heads"]

    def per_device(tokens, norm_gain, w_query, w_key, w_value, head_gain, w_out):
        rows, depth = tokens.shape
        heads = w_query.shape[1] // HD
        width = w_out.shape[1]
        cw = width // nh
        subs = 2
        sw = cw // subs
        pairs = nh // 2
        group = n // heads
        per = 2 if heads % 2 == 0 else 1
        bf = jnp.bfloat16
        dma = pltpu.SemaphoreType.DMA
        hbm = pl.BlockSpec(memory_space=pltpu.HBM)
        vmem = pl.BlockSpec(memory_space=pltpu.VMEM)
        return pl.pallas_call(
            functools.partial(fused_kernel, n, nh),
            out_shape=jax.ShapeDtypeStruct((rows, cw), bf),
            in_specs=[hbm, vmem, hbm, hbm, hbm, vmem, hbm],
            out_specs=vmem,
            scratch_shapes=[
                pltpu.VMEM((rows, depth), bf),
                pltpu.VMEM((rows, depth), bf),
                pltpu.VMEM((heads, depth, 2 * HD), bf),
                pltpu.VMEM((heads // per, depth, per * HD), bf),
                pltpu.VMEM(w_out.shape, bf),
                pltpu.VMEM((heads, rows, 2 * HD), bf),
                pltpu.VMEM((heads, rows, HD), bf),
                pltpu.VMEM((n, rows, 2 * HD), bf),
                pltpu.VMEM((heads, rows, HD), bf),
                pltpu.VMEM((heads, rows, HD), bf),
                pltpu.VMEM((rows, heads * HD), bf),
                pltpu.VMEM((pairs, subs, rows, sw), bf),
                pltpu.VMEM((pairs, subs, rows, sw), bf),
                pltpu.VMEM((pairs - 1, subs, rows, sw), bf),
                pltpu.VMEM((pairs - 1, subs, rows, sw), bf),
                pltpu.VMEM((subs, rows, sw), jnp.float32),
                dma,
                dma((heads, 3)),
                dma,
                dma((heads,)),
                dma((heads,)),
                dma((heads, group)),
                dma((n,)),
                dma((heads,)),
                dma((heads,)),
                dma((heads,)),
                dma((pairs, subs)),
                dma((pairs, subs)),
                dma((pairs - 1, subs)),
                dma((pairs - 1, subs)),
            ],
            compiler_params=pltpu.CompilerParams(
                collective_id=0, has_side_effects=True, vmem_limit_bytes=60 * 1024 * 1024
            ),
            name="fused_block",
        )(tokens, norm_gain[None, :], w_query, w_key, w_value, head_gain[None, :], w_out)

    placed = (
        P("frames", None),
        P(),
        P(None, "heads"),
        P(None, "heads"),
        P(None, "heads"),
        P("heads"),
        P("heads", None),
    )
    return jax.shard_map(
        per_device, mesh=mesh, in_specs=placed, out_specs=P("frames", "heads"), check_vma=False
    )
```

```python
import functools
import math

import jax
import jax.numpy as jnp
from jax import lax
from jax.experimental import pallas as pl
from jax.experimental.pallas import tpu as pltpu
from jax.sharding import PartitionSpec as P

HD = 128
EPS = 1e-06
MESH = pl.DeviceIdType.MESH


def fused_kernel(
    n, nh,
    tokens_hbm, norm_gain_ref, wq_hbm, wk_hbm, wv_hbm, head_gain_ref, wo_hbm,
    out_ref,
    tok, normed, wkv, wq, wo, kvout, qout, kv, q, oout, headed, s1, r1, s2, r2, acc,
    tok_sem, w_sem, wo_sem,
    kvs_sem, qs_sem, fw_sem, kvr_sem, qr_sem, os_sem, or_sem,
    s1_sem, r1_sem, s2_sem, r2_sem,
):
    heads = kvout.shape[0]
    rows = tok.shape[0]
    group = n // heads
    half = max(heads // 2, 1)
    me = lax.axis_index("frames")
    lane = lax.axis_index("heads")
    level, member = lax.div(me, group), lax.rem(me, group)
    core, pair = lax.rem(lane, 2), lax.div(lane, 2)
    pairs = nh // 2
    lower = level < half

    def head_at(k):
        return jnp.where(lower, heads - 1 - k, k)

    tok_copy = pltpu.make_async_copy(tokens_hbm, tok, tok_sem)
    tok_copy.start()
    loads = []
    per = 2 if heads % 2 == 0 else 1
    for k in range(heads):
        cols = pl.ds(pl.multiple_of(head_at(k) * HD, HD), HD)
        loads.append((
            pltpu.make_async_copy(wk_hbm.at[:, cols], wkv.at[k, :, pl.ds(0, HD)], w_sem.at[k, 0]),
            pltpu.make_async_copy(wv_hbm.at[:, cols], wkv.at[k, :, pl.ds(HD, HD)], w_sem.at[k, 1]),
            pltpu.make_async_copy(
                wq_hbm.at[:, cols], wq.at[k // per, :, pl.ds((k % per) * HD, HD)], w_sem.at[k, 2]
            ),
        ))
    loads[0][0].start()
    loads[0][1].start()

    barrier = pltpu.get_barrier_semaphore()
    for d in range(1, heads):
        other = lax.rem(level + d, heads) * group + member
        pl.semaphore_signal(barrier, inc=1, device_id={"frames": other}, device_id_type=MESH)
    for d in range(1, group):
        other = level * group + lax.rem(member + d, group)
        pl.semaphore_signal(barrier, inc=1, device_id={"frames": other}, device_id_type=MESH)
    mate = pair * 2 + 1 - core
    pl.semaphore_signal(barrier, inc=1, device_id={"heads": mate}, device_id_type=MESH)
    for d in range(1, pairs):
        other = lax.rem(pair + d, pairs) * 2 + core
        pl.semaphore_signal(barrier, inc=1, device_id={"heads": other}, device_id_type=MESH)

    tok_copy.wait()
    for k in range(1, heads):
        loads[k][0].start()
        loads[k][1].start()
    for k in range(heads):
        loads[k][2].start()
    wo_copy = pltpu.make_async_copy(wo_hbm, wo, wo_sem)
    wo_copy.start()
    for start in range(0, rows, 32):
        part = pl.ds(start, 32)
        wide = tok[part, :].astype(jnp.float32)
        scale = lax.rsqrt(jnp.mean(wide * wide, axis=1, keepdims=True) + EPS)
        normed[part, :] = (wide * scale * norm_gain_ref[...]).astype(jnp.bfloat16)

    pl.semaphore_wait(barrier, heads - 1 + group - 1 + 1 + pairs - 1)

    def kv_send(k, target):
        return pltpu.make_async_remote_copy(
            src_ref=kvout.at[k], dst_ref=kv.at[me],
            send_sem=kvs_sem.at[k], recv_sem=kvr_sem.at[me],
            device_id={"frames": target}, device_id_type=MESH,
        )

    def q_send(k, target):
        return pltpu.make_async_remote_copy(
            src_ref=qout.at[k], dst_ref=q.at[level],
            send_sem=qs_sem.at[k], recv_sem=qr_sem.at[level],
            device_id={"frames": target}, device_id_type=MESH,
        )

    def forward(source, d):
        target = level * group + lax.rem(member + d, group)
        return pltpu.make_async_remote_copy(
            src_ref=kv.at[source], dst_ref=kv.at[source],
            send_sem=fw_sem.at[lax.div(source, group), d], recv_sem=kvr_sem.at[source],
            device_id={"frames": target}, device_id_type=MESH,
        )

    def kv_arrived(source):
        return pltpu.make_async_remote_copy(
            src_ref=kv.at[source], dst_ref=kv.at[source],
            send_sem=kvs_sem.at[0], recv_sem=kvr_sem.at[source],
            device_id={"frames": me}, device_id_type=MESH,
        )

    def q_arrived(source):
        return pltpu.make_async_remote_copy(
            src_ref=q.at[source], dst_ref=q.at[source],
            send_sem=qs_sem.at[0], recv_sem=qr_sem.at[source],
            device_id={"frames": me}, device_id_type=MESH,
        )

    for k in range(heads):
        loads[k][0].wait()
        loads[k][1].wait()
        block = jnp.dot(normed[...], wkv[k], preferred_element_type=jnp.float32)
        block = block.astype(jnp.bfloat16)
        h = head_at(k)

        @pl.when(h != level)
        def _():
            kvout[k] = block
            kv_send(k, h * group + member).start()

        @pl.when(h == level)
        def _():
            kv[me] = block
            for d in range(1, group):
                forward(me, d).start()

    for first in range(0, heads, per):
        for k in range(first, first + per):
            loads[k][2].wait()
        block = jnp.dot(normed[...], wq[first // per], preferred_element_type=jnp.float32)
        block = block.astype(jnp.bfloat16)
        for k in range(first, first + per):
            h = head_at(k)
            part = block[:, (k - first) * HD : (k - first + 1) * HD]

            @pl.when(h != level)
            def _():
                qout[k] = part
                q_send(k, h * group + member).start()

            @pl.when(h == level)
            def _():
                q[level] = part

    inner = (level == half) | (level == half - 1)
    turn = jnp.where(inner, half, 0)
    for d in range(heads):
        step = lax.rem(turn + d, heads)
        src_level = jnp.where(
            lower, lax.rem(half + step, heads), lax.rem(half - 1 - step + heads, heads)
        )
        source = src_level * group + member

        @pl.when(src_level != level)
        def _():
            kv_arrived(source).wait_recv()
            for e in range(1, group):
                forward(source, e).start()

    def o_send(i):
        return pltpu.make_async_remote_copy(
            src_ref=oout.at[i],
            dst_ref=headed.at[:, pl.ds(pl.multiple_of(level * HD, HD), HD)],
            send_sem=os_sem.at[i], recv_sem=or_sem.at[level],
            device_id={"frames": i * group + member}, device_id_type=MESH,
        )

    inv_root = 1.0 / math.sqrt(HD)
    gain = head_gain_ref[:, pl.ds(pl.multiple_of(level * HD, HD), HD)]
    for i in range(heads):
        for d in range(1, group):
            kv_arrived(i * group + lax.rem(member + d, group)).wait_recv()

        @pl.when(level != i)
        def _():
            q_arrived(i).wait_recv()

        reach = (i + 1) * group
        keys = kv[:reach, :, :HD].reshape(reach * rows, HD)
        values = kv[:reach, :, HD:].reshape(reach * rows, HD)
        scores = lax.dot_general(
            q[i], keys, (((1,), (1,)), ((), ())), preferred_element_type=jnp.float32
        ) * inv_root
        query_pos = (i * group + member) * rows + lax.broadcasted_iota(jnp.int32, scores.shape, 0)
        key_pos = lax.broadcasted_iota(jnp.int32, scores.shape, 1)
        scores = jnp.where(key_pos <= query_pos, scores, jnp.float32(-1e30))
        top = jnp.max(scores, axis=1, keepdims=True)
        weights = jnp.exp(scores - top)
        total = jnp.sum(weights, axis=1, keepdims=True)
        attended = jnp.dot(
            weights.astype(jnp.bfloat16), values, preferred_element_type=jnp.float32
        ) / total
        scale = lax.rsqrt(jnp.mean(attended * attended, axis=1, keepdims=True) + EPS)
        result = (attended * scale * gain).astype(jnp.bfloat16)

        @pl.when(level != i)
        def _():
            oout[i] = result
            o_send(i).start()

        @pl.when(level == i)
        def _():
            headed[:, pl.ds(pl.multiple_of(level * HD, HD), HD)] = result

    wo_copy.wait()
    for h in range(heads):
        @pl.when(level != h)
        def _():
            here = headed.at[:, pl.ds(h * HD, HD)]
            pltpu.make_async_remote_copy(
                src_ref=here, dst_ref=here, send_sem=os_sem.at[0], recv_sem=or_sem.at[h],
                device_id={"frames": me}, device_id_type=MESH,
            ).wait_recv()

    cw = out_ref.shape[1]
    subs, sw = s1.shape[1], s1.shape[3]
    heads_in = headed[...]

    def partial_at(d, side, s):
        to = lax.rem(pair + d, pairs) * 2 + side
        cols = pl.ds(pl.multiple_of(to * cw + s * sw, sw), sw)
        return jnp.dot(heads_in, wo[:, cols], preferred_element_type=jnp.float32)

    def mate_send(d, s):
        return pltpu.make_async_remote_copy(
            src_ref=s1.at[d, s], dst_ref=r1.at[d, s],
            send_sem=s1_sem.at[d, s], recv_sem=r1_sem.at[d, s],
            device_id={"heads": mate}, device_id_type=MESH,
        )

    def pair_send(d, s):
        return pltpu.make_async_remote_copy(
            src_ref=s2.at[d - 1, s], dst_ref=r2.at[d - 1, s],
            send_sem=s2_sem.at[d - 1, s], recv_sem=r2_sem.at[d - 1, s],
            device_id={"heads": lax.rem(pair + d, pairs) * 2 + core}, device_id_type=MESH,
        )

    order = [(d % pairs, s) for d in range(1, pairs + 1) for s in range(subs)]
    for to in range(1, pairs + 1):
        d = to % pairs
        for s in range(subs):
            s1[d, s] = partial_at(d, 1 - core, s).astype(jnp.bfloat16)
            mate_send(d, s).start()
        for s in range(subs):
            own = partial_at(d, core, s)
            mate_send(d, s).wait_recv()
            own = own + r1[d, s].astype(jnp.float32)
            if d:
                s2[d - 1, s] = own.astype(jnp.bfloat16)
                pair_send(d, s).start()
            else:
                acc[s] = own
    for s in range(subs):
        whole = acc[s]
        for d in range(1, pairs):
            pair_send(d, s).wait_recv()
            whole = whole + r2[d - 1, s].astype(jnp.float32)
        out_ref[:, s * sw : (s + 1) * sw] = whole.astype(jnp.bfloat16)

    for d, s in order:
        mate_send(d, s).wait_send()
        if d:
            pair_send(d, s).wait_send()
    for i in range(heads):
        @pl.when(level != i)
        def _():
            o_send(i).wait_send()

        for d in range(1, group):
            forward(i * group + member, d).wait_send()
    for k in range(heads):
        @pl.when(head_at(k) != level)
        def _():
            kv_send(k, head_at(k) * group + member).wait_send()
            q_send(k, head_at(k) * group + member).wait_send()


def solution(mesh):
    n, nh = mesh.shape["frames"], mesh.shape["heads"]

    def per_device(tokens, norm_gain, w_query, w_key, w_value, head_gain, w_out):
        rows, depth = tokens.shape
        heads = w_query.shape[1] // HD
        width = w_out.shape[1]
        cw = width // nh
        subs = 4
        sw = cw // subs
        pairs = nh // 2
        group = n // heads
        per = 2 if heads % 2 == 0 else 1
        bf = jnp.bfloat16
        dma = pltpu.SemaphoreType.DMA
        hbm = pl.BlockSpec(memory_space=pltpu.HBM)
        vmem = pl.BlockSpec(memory_space=pltpu.VMEM)
        return pl.pallas_call(
            functools.partial(fused_kernel, n, nh),
            out_shape=jax.ShapeDtypeStruct((rows, cw), bf),
            in_specs=[hbm, vmem, hbm, hbm, hbm, vmem, hbm],
            out_specs=vmem,
            scratch_shapes=[
                pltpu.VMEM((rows, depth), bf),
                pltpu.VMEM((rows, depth), bf),
                pltpu.VMEM((heads, depth, 2 * HD), bf),
                pltpu.VMEM((heads // per, depth, per * HD), bf),
                pltpu.VMEM(w_out.shape, bf),
                pltpu.VMEM((heads, rows, 2 * HD), bf),
                pltpu.VMEM((heads, rows, HD), bf),
                pltpu.VMEM((n, rows, 2 * HD), bf),
                pltpu.VMEM((heads, rows, HD), bf),
                pltpu.VMEM((heads, rows, HD), bf),
                pltpu.VMEM((rows, heads * HD), bf),
                pltpu.VMEM((pairs, subs, rows, sw), bf),
                pltpu.VMEM((pairs, subs, rows, sw), bf),
                pltpu.VMEM((pairs - 1, subs, rows, sw), bf),
                pltpu.VMEM((pairs - 1, subs, rows, sw), bf),
                pltpu.VMEM((subs, rows, sw), jnp.float32),
                dma,
                dma((heads, 3)),
                dma,
                dma((heads,)),
                dma((heads,)),
                dma((heads, group)),
                dma((n,)),
                dma((heads,)),
                dma((heads,)),
                dma((heads,)),
                dma((pairs, subs)),
                dma((pairs, subs)),
                dma((pairs - 1, subs)),
                dma((pairs - 1, subs)),
            ],
            compiler_params=pltpu.CompilerParams(
                collective_id=0, has_side_effects=True, vmem_limit_bytes=60 * 1024 * 1024
            ),
            name="fused_block",
        )(tokens, norm_gain[None, :], w_query, w_key, w_value, head_gain[None, :], w_out)

    placed = (
        P("frames", None),
        P(),
        P(None, "heads"),
        P(None, "heads"),
        P(None, "heads"),
        P("heads"),
        P("heads", None),
    )
    return jax.shard_map(
        per_device, mesh=mesh, in_specs=placed, out_specs=P("frames", "heads"), check_vma=False
    )
```

```python
import functools
import math

import jax
import jax.numpy as jnp
from jax import lax
from jax.experimental import pallas as pl
from jax.experimental.pallas import tpu as pltpu
from jax.sharding import PartitionSpec as P

HD = 128
EPS = 1e-06
MESH = pl.DeviceIdType.MESH


def fused_kernel(
    n, nh,
    tokens_hbm, norm_gain_ref, wq_hbm, wk_hbm, wv_hbm, head_gain_ref, wo_hbm,
    out_ref,
    tok, normed, wkv, wq, wo, kvout, qout, kv, q, oout, headed, s1, r1, s2, r2, acc,
    tok_sem, w_sem, wo_sem,
    kvs_sem, qs_sem, fw_sem, kvr_sem, qr_sem, os_sem, or_sem,
    s1_sem, r1_sem, s2_sem, r2_sem,
):
    heads = kvout.shape[0]
    rows = tok.shape[0]
    group = n // heads
    half = max(heads // 2, 1)
    me = lax.axis_index("frames")
    lane = lax.axis_index("heads")
    level, member = lax.div(me, group), lax.rem(me, group)
    core, pair = lax.rem(lane, 2), lax.div(lane, 2)
    pairs = nh // 2
    lower = level < half

    def head_at(k):
        return jnp.where(lower, heads - 1 - k, k)

    tok_copy = pltpu.make_async_copy(tokens_hbm, tok, tok_sem)
    tok_copy.start()
    loads = []
    per = 2 if heads % 2 == 0 else 1
    for k in range(heads):
        cols = pl.ds(pl.multiple_of(head_at(k) * HD, HD), HD)
        loads.append((
            pltpu.make_async_copy(wk_hbm.at[:, cols], wkv.at[k, :, pl.ds(0, HD)], w_sem.at[k, 0]),
            pltpu.make_async_copy(wv_hbm.at[:, cols], wkv.at[k, :, pl.ds(HD, HD)], w_sem.at[k, 1]),
            pltpu.make_async_copy(
                wq_hbm.at[:, cols], wq.at[k // per, :, pl.ds((k % per) * HD, HD)], w_sem.at[k, 2]
            ),
        ))
    loads[0][0].start()
    loads[0][1].start()

    barrier = pltpu.get_barrier_semaphore()
    for d in range(1, heads):
        other = lax.rem(level + d, heads) * group + member
        pl.semaphore_signal(barrier, inc=1, device_id={"frames": other}, device_id_type=MESH)
    for d in range(1, group):
        other = level * group + lax.rem(member + d, group)
        pl.semaphore_signal(barrier, inc=1, device_id={"frames": other}, device_id_type=MESH)
    mate = pair * 2 + 1 - core
    pl.semaphore_signal(barrier, inc=1, device_id={"heads": mate}, device_id_type=MESH)
    for d in range(1, pairs):
        other = lax.rem(pair + d, pairs) * 2 + core
        pl.semaphore_signal(barrier, inc=1, device_id={"heads": other}, device_id_type=MESH)

    tok_copy.wait()
    for k in range(1, heads):
        loads[k][0].start()
        loads[k][1].start()
    for k in range(heads):
        loads[k][2].start()
    wo_copy = pltpu.make_async_copy(wo_hbm, wo, wo_sem)
    wo_copy.start()
    for start in range(0, rows, 32):
        part = pl.ds(start, 32)
        wide = tok[part, :].astype(jnp.float32)
        scale = lax.rsqrt(jnp.mean(wide * wide, axis=1, keepdims=True) + EPS)
        normed[part, :] = (wide * scale * norm_gain_ref[...]).astype(jnp.bfloat16)

    pl.semaphore_wait(barrier, heads - 1 + group - 1 + 1 + pairs - 1)

    def kv_send(k, target):
        return pltpu.make_async_remote_copy(
            src_ref=kvout.at[k], dst_ref=kv.at[me],
            send_sem=kvs_sem.at[k], recv_sem=kvr_sem.at[me],
            device_id={"frames": target}, device_id_type=MESH,
        )

    def q_send(k, target):
        return pltpu.make_async_remote_copy(
            src_ref=qout.at[k], dst_ref=q.at[level],
            send_sem=qs_sem.at[k], recv_sem=qr_sem.at[level],
            device_id={"frames": target}, device_id_type=MESH,
        )

    def forward(source, d):
        target = level * group + lax.rem(member + d, group)
        return pltpu.make_async_remote_copy(
            src_ref=kv.at[source], dst_ref=kv.at[source],
            send_sem=fw_sem.at[lax.div(source, group), d], recv_sem=kvr_sem.at[source],
            device_id={"frames": target}, device_id_type=MESH,
        )

    def kv_arrived(source):
        return pltpu.make_async_remote_copy(
            src_ref=kv.at[source], dst_ref=kv.at[source],
            send_sem=kvs_sem.at[0], recv_sem=kvr_sem.at[source],
            device_id={"frames": me}, device_id_type=MESH,
        )

    def q_arrived(source):
        return pltpu.make_async_remote_copy(
            src_ref=q.at[source], dst_ref=q.at[source],
            send_sem=qs_sem.at[0], recv_sem=qr_sem.at[source],
            device_id={"frames": me}, device_id_type=MESH,
        )

    for k in range(heads):
        loads[k][0].wait()
        loads[k][1].wait()
        block = jnp.dot(normed[...], wkv[k], preferred_element_type=jnp.float32)
        block = block.astype(jnp.bfloat16)
        h = head_at(k)

        @pl.when(h != level)
        def _():
            kvout[k] = block
            kv_send(k, h * group + member).start()

        @pl.when(h == level)
        def _():
            kv[me] = block
            for d in range(1, group):
                forward(me, d).start()

    for first in range(0, heads, per):
        for k in range(first, first + per):
            loads[k][2].wait()
        block = jnp.dot(normed[...], wq[first // per], preferred_element_type=jnp.float32)
        block = block.astype(jnp.bfloat16)
        for k in range(first, first + per):
            h = head_at(k)
            part = block[:, (k - first) * HD : (k - first + 1) * HD]

            @pl.when(h != level)
            def _():
                qout[k] = part
                q_send(k, h * group + member).start()

            @pl.when(h == level)
            def _():
                q[level] = part

    inner = (level == half) | (level == half - 1)
    turn = jnp.where(inner, half, 0)
    for d in range(heads):
        step = lax.rem(turn + d, heads)
        src_level = jnp.where(
            lower, lax.rem(half + step, heads), lax.rem(half - 1 - step + heads, heads)
        )
        source = src_level * group + member

        @pl.when(src_level != level)
        def _():
            kv_arrived(source).wait_recv()
            for e in range(1, group):
                forward(source, e).start()

    def o_send(i):
        return pltpu.make_async_remote_copy(
            src_ref=oout.at[i],
            dst_ref=headed.at[:, pl.ds(pl.multiple_of(level * HD, HD), HD)],
            send_sem=os_sem.at[i], recv_sem=or_sem.at[level],
            device_id={"frames": i * group + member}, device_id_type=MESH,
        )

    inv_root = 1.0 / math.sqrt(HD)
    gain = head_gain_ref[:, pl.ds(pl.multiple_of(level * HD, HD), HD)]
    for i in range(heads):
        for d in range(1, group):
            kv_arrived(i * group + lax.rem(member + d, group)).wait_recv()

        @pl.when(level != i)
        def _():
            q_arrived(i).wait_recv()

        reach = (i + 1) * group
        keys = kv[:reach, :, :HD].reshape(reach * rows, HD)
        values = kv[:reach, :, HD:].reshape(reach * rows, HD)
        scores = lax.dot_general(
            q[i], keys, (((1,), (1,)), ((), ())), preferred_element_type=jnp.float32
        ) * inv_root
        query_pos = (i * group + member) * rows + lax.broadcasted_iota(jnp.int32, scores.shape, 0)
        key_pos = lax.broadcasted_iota(jnp.int32, scores.shape, 1)
        scores = jnp.where(key_pos <= query_pos, scores, jnp.float32(-1e30))
        top = jnp.max(scores, axis=1, keepdims=True)
        weights = jnp.exp(scores - top)
        total = jnp.sum(weights, axis=1, keepdims=True)
        attended = jnp.dot(
            weights.astype(jnp.bfloat16), values, preferred_element_type=jnp.float32
        ) / total
        scale = lax.rsqrt(jnp.mean(attended * attended, axis=1, keepdims=True) + EPS)
        result = (attended * scale * gain).astype(jnp.bfloat16)

        @pl.when(level != i)
        def _():
            oout[i] = result
            o_send(i).start()

        @pl.when(level == i)
        def _():
            headed[:, pl.ds(pl.multiple_of(level * HD, HD), HD)] = result

    wo_copy.wait()
    for h in range(heads):
        @pl.when(level != h)
        def _():
            here = headed.at[:, pl.ds(h * HD, HD)]
            pltpu.make_async_remote_copy(
                src_ref=here, dst_ref=here, send_sem=os_sem.at[0], recv_sem=or_sem.at[h],
                device_id={"frames": me}, device_id_type=MESH,
            ).wait_recv()

    cw = out_ref.shape[1]
    subs, sw = s1.shape[1], s1.shape[3]
    heads_in = headed[...]

    def partial_at(d, side, s):
        to = lax.rem(pair + d, pairs) * 2 + side
        cols = pl.ds(pl.multiple_of(to * cw + s * sw, sw), sw)
        return jnp.dot(heads_in, wo[:, cols], preferred_element_type=jnp.float32)

    def mate_send(d, s):
        return pltpu.make_async_remote_copy(
            src_ref=s1.at[d, s], dst_ref=r1.at[d, s],
            send_sem=s1_sem.at[d, s], recv_sem=r1_sem.at[d, s],
            device_id={"heads": mate}, device_id_type=MESH,
        )

    def pair_send(d, s):
        return pltpu.make_async_remote_copy(
            src_ref=s2.at[d - 1, s], dst_ref=r2.at[d - 1, s],
            send_sem=s2_sem.at[d - 1, s], recv_sem=r2_sem.at[d - 1, s],
            device_id={"heads": lax.rem(pair + d, pairs) * 2 + core}, device_id_type=MESH,
        )

    order = [(d % pairs, s) for d in range(1, pairs + 1) for s in range(subs)]
    for to in range(1, pairs + 1):
        d = to % pairs
        for s in range(subs):
            s1[d, s] = partial_at(d, 1 - core, s).astype(jnp.bfloat16)
            mate_send(d, s).start()
        for s in range(subs):
            own = partial_at(d, core, s)
            mate_send(d, s).wait_recv()
            own = own + r1[d, s].astype(jnp.float32)
            if d:
                s2[d - 1, s] = own.astype(jnp.bfloat16)
                pair_send(d, s).start()
            else:
                acc[s] = own
    for s in range(subs):
        whole = acc[s]
        for d in range(1, pairs):
            pair_send(d, s).wait_recv()
            whole = whole + r2[d - 1, s].astype(jnp.float32)
        out_ref[:, s * sw : (s + 1) * sw] = whole.astype(jnp.bfloat16)

    for d, s in order:
        mate_send(d, s).wait_send()
        if d:
            pair_send(d, s).wait_send()
    for i in range(heads):
        @pl.when(level != i)
        def _():
            o_send(i).wait_send()

        for d in range(1, group):
            forward(i * group + member, d).wait_send()
    for k in range(heads):
        @pl.when(head_at(k) != level)
        def _():
            kv_send(k, head_at(k) * group + member).wait_send()
            q_send(k, head_at(k) * group + member).wait_send()


def solution(mesh):
    n, nh = mesh.shape["frames"], mesh.shape["heads"]

    def per_device(tokens, norm_gain, w_query, w_key, w_value, head_gain, w_out):
        rows, depth = tokens.shape
        heads = w_query.shape[1] // HD
        width = w_out.shape[1]
        cw = width // nh
        subs = 4
        sw = cw // subs
        pairs = nh // 2
        group = n // heads
        per = 2 if heads % 2 == 0 else 1
        bf = jnp.bfloat16
        dma = pltpu.SemaphoreType.DMA
        hbm = pl.BlockSpec(memory_space=pltpu.HBM)
        vmem = pl.BlockSpec(memory_space=pltpu.VMEM)
        return pl.pallas_call(
            functools.partial(fused_kernel, n, nh),
            out_shape=jax.ShapeDtypeStruct((rows, cw), bf),
            in_specs=[hbm, vmem, hbm, hbm, hbm, vmem, hbm],
            out_specs=vmem,
            scratch_shapes=[
                pltpu.VMEM((rows, depth), bf),
                pltpu.VMEM((rows, depth), bf),
                pltpu.VMEM((heads, depth, 2 * HD), bf),
                pltpu.VMEM((heads // per, depth, per * HD), bf),
                pltpu.VMEM(w_out.shape, bf),
                pltpu.VMEM((heads, rows, 2 * HD), bf),
                pltpu.VMEM((heads, rows, HD), bf),
                pltpu.VMEM((n, rows, 2 * HD), bf),
                pltpu.VMEM((heads, rows, HD), bf),
                pltpu.VMEM((heads, rows, HD), bf),
                pltpu.VMEM((rows, heads * HD), bf),
                pltpu.VMEM((pairs, subs, rows, sw), bf),
                pltpu.VMEM((pairs, subs, rows, sw), bf),
                pltpu.VMEM((pairs - 1, subs, rows, sw), bf),
                pltpu.VMEM((pairs - 1, subs, rows, sw), bf),
                pltpu.VMEM((subs, rows, sw), jnp.float32),
                dma,
                dma((heads, 3)),
                dma,
                dma((heads,)),
                dma((heads,)),
                dma((heads, group)),
                dma((n,)),
                dma((heads,)),
                dma((heads,)),
                dma((heads,)),
                dma((pairs, subs)),
                dma((pairs, subs)),
                dma((pairs - 1, subs)),
                dma((pairs - 1, subs)),
            ],
            compiler_params=pltpu.CompilerParams(
                collective_id=0, has_side_effects=True, vmem_limit_bytes=55783424
            ),
            name="fused_block",
        )(tokens, norm_gain[None, :], w_query, w_key, w_value, head_gain[None, :], w_out)

    placed = (
        P("frames", None),
        P(),
        P(None, "heads"),
        P(None, "heads"),
        P(None, "heads"),
        P("heads"),
        P("heads", None),
    )
    return jax.shard_map(
        per_device, mesh=mesh, in_specs=placed, out_specs=P("frames", "heads"), check_vma=False
    )
```

```python
import functools
import math

import jax
import jax.numpy as jnp
from jax import lax
from jax.experimental import pallas as pl
from jax.experimental.pallas import tpu as pltpu
from jax.sharding import PartitionSpec as P

HD = 128
EPS = 1e-06
MESH = pl.DeviceIdType.MESH


def fused_kernel(
    n, nh,
    tokens_hbm, norm_gain_ref, wq_hbm, wk_hbm, wv_hbm, head_gain_ref, wo_hbm,
    out_ref,
    tok, normed, wkv, wq, wo, kvout, qout, kv, q, oout, headed, s1, r1, s2, r2, acc,
    tok_sem, w_sem, wo_sem,
    kvs_sem, qs_sem, fw_sem, kvr_sem, qr_sem, os_sem, or_sem,
    s1_sem, r1_sem, s2_sem, r2_sem,
):
    heads = kvout.shape[0]
    rows = tok.shape[0]
    group = n // heads
    half = max(heads // 2, 1)
    me = lax.axis_index("frames")
    lane = lax.axis_index("heads")
    level, member = lax.div(me, group), lax.rem(me, group)
    core, pair = lax.rem(lane, 2), lax.div(lane, 2)
    pairs = nh // 2
    lower = level < half

    def head_at(k):
        return jnp.where(lower, heads - 1 - k, k)

    tok_copy = pltpu.make_async_copy(tokens_hbm, tok, tok_sem)
    tok_copy.start()
    loads = []
    per = 2 if heads % 2 == 0 else 1
    for k in range(heads):
        cols = pl.ds(pl.multiple_of(head_at(k) * HD, HD), HD)
        loads.append((
            pltpu.make_async_copy(wk_hbm.at[:, cols], wkv.at[k, :, pl.ds(0, HD)], w_sem.at[k, 0]),
            pltpu.make_async_copy(wv_hbm.at[:, cols], wkv.at[k, :, pl.ds(HD, HD)], w_sem.at[k, 1]),
            pltpu.make_async_copy(
                wq_hbm.at[:, cols], wq.at[k // per, :, pl.ds((k % per) * HD, HD)], w_sem.at[k, 2]
            ),
        ))
    loads[0][0].start()
    loads[0][1].start()

    barrier = pltpu.get_barrier_semaphore()
    for d in range(1, heads):
        other = lax.rem(level + d, heads) * group + member
        pl.semaphore_signal(barrier, inc=1, device_id={"frames": other}, device_id_type=MESH)
    for d in range(1, group):
        other = level * group + lax.rem(member + d, group)
        pl.semaphore_signal(barrier, inc=1, device_id={"frames": other}, device_id_type=MESH)
    mate = pair * 2 + 1 - core
    pl.semaphore_signal(barrier, inc=1, device_id={"heads": mate}, device_id_type=MESH)
    for d in range(1, pairs):
        other = lax.rem(pair + d, pairs) * 2 + core
        pl.semaphore_signal(barrier, inc=1, device_id={"heads": other}, device_id_type=MESH)

    tok_copy.wait()
    for k in range(1, heads):
        loads[k][0].start()
        loads[k][1].start()
    for k in range(heads):
        loads[k][2].start()
    wo_copy = pltpu.make_async_copy(wo_hbm, wo, wo_sem)
    wo_copy.start()
    for start in range(0, rows, 32):
        part = pl.ds(start, 32)
        wide = tok[part, :].astype(jnp.float32)
        scale = lax.rsqrt(jnp.mean(wide * wide, axis=1, keepdims=True) + EPS)
        normed[part, :] = (wide * scale * norm_gain_ref[...]).astype(jnp.bfloat16)

    pl.semaphore_wait(barrier, heads - 1 + group - 1 + 1 + pairs - 1)

    def kv_send(k, target):
        return pltpu.make_async_remote_copy(
            src_ref=kvout.at[k], dst_ref=kv.at[me],
            send_sem=kvs_sem.at[k], recv_sem=kvr_sem.at[me],
            device_id={"frames": target}, device_id_type=MESH,
        )

    def q_send(k, target):
        return pltpu.make_async_remote_copy(
            src_ref=qout.at[k], dst_ref=q.at[level],
            send_sem=qs_sem.at[k], recv_sem=qr_sem.at[level],
            device_id={"frames": target}, device_id_type=MESH,
        )

    def forward(source, d):
        target = level * group + lax.rem(member + d, group)
        return pltpu.make_async_remote_copy(
            src_ref=kv.at[source], dst_ref=kv.at[source],
            send_sem=fw_sem.at[lax.div(source, group), d], recv_sem=kvr_sem.at[source],
            device_id={"frames": target}, device_id_type=MESH,
        )

    def kv_arrived(source):
        return pltpu.make_async_remote_copy(
            src_ref=kv.at[source], dst_ref=kv.at[source],
            send_sem=kvs_sem.at[0], recv_sem=kvr_sem.at[source],
            device_id={"frames": me}, device_id_type=MESH,
        )

    def q_arrived(source):
        return pltpu.make_async_remote_copy(
            src_ref=q.at[source], dst_ref=q.at[source],
            send_sem=qs_sem.at[0], recv_sem=qr_sem.at[source],
            device_id={"frames": me}, device_id_type=MESH,
        )

    for k in range(heads):
        loads[k][0].wait()
        loads[k][1].wait()
        block = jnp.dot(normed[...], wkv[k], preferred_element_type=jnp.float32)
        block = block.astype(jnp.bfloat16)
        h = head_at(k)

        @pl.when(h != level)
        def _():
            kvout[k] = block
            kv_send(k, h * group + member).start()

        @pl.when(h == level)
        def _():
            kv[me] = block
            for d in range(1, group):
                forward(me, d).start()

    for first in range(0, heads, per):
        for k in range(first, first + per):
            loads[k][2].wait()
        block = jnp.dot(normed[...], wq[first // per], preferred_element_type=jnp.float32)
        block = block.astype(jnp.bfloat16)
        for k in range(first, first + per):
            h = head_at(k)
            part = block[:, (k - first) * HD : (k - first + 1) * HD]

            @pl.when(h != level)
            def _():
                qout[k] = part
                q_send(k, h * group + member).start()

            @pl.when(h == level)
            def _():
                q[level] = part

    inner = (level == half) | (level == half - 1)
    turn = jnp.where(inner, half, 0)
    for d in range(heads):
        step = lax.rem(turn + d, heads)
        src_level = jnp.where(
            lower, lax.rem(half + step, heads), lax.rem(half - 1 - step + heads, heads)
        )
        source = src_level * group + member

        @pl.when(src_level != level)
        def _():
            kv_arrived(source).wait_recv()
            for e in range(1, group):
                forward(source, e).start()

    def o_send(i):
        return pltpu.make_async_remote_copy(
            src_ref=oout.at[i],
            dst_ref=headed.at[:, pl.ds(pl.multiple_of(level * HD, HD), HD)],
            send_sem=os_sem.at[i], recv_sem=or_sem.at[level],
            device_id={"frames": i * group + member}, device_id_type=MESH,
        )

    inv_root = 1.0 / math.sqrt(HD)
    gain = head_gain_ref[:, pl.ds(pl.multiple_of(level * HD, HD), HD)]
    for i in range(heads):
        for d in range(1, group):
            kv_arrived(i * group + lax.rem(member + d, group)).wait_recv()

        @pl.when(level != i)
        def _():
            q_arrived(i).wait_recv()

        reach = (i + 1) * group
        keys = kv[:reach, :, :HD].reshape(reach * rows, HD)
        values = kv[:reach, :, HD:].reshape(reach * rows, HD)
        scores = lax.dot_general(
            q[i], keys, (((1,), (1,)), ((), ())), preferred_element_type=jnp.float32
        ) * inv_root
        query_pos = (i * group + member) * rows + lax.broadcasted_iota(jnp.int32, scores.shape, 0)
        key_pos = lax.broadcasted_iota(jnp.int32, scores.shape, 1)
        scores = jnp.where(key_pos <= query_pos, scores, jnp.float32(-1e30))
        top = jnp.max(scores, axis=1, keepdims=True)
        weights = jnp.exp(scores - top)
        total = jnp.sum(weights, axis=1, keepdims=True)
        attended = jnp.dot(
            weights.astype(jnp.bfloat16), values, preferred_element_type=jnp.float32
        ) / total
        scale = lax.rsqrt(jnp.mean(attended * attended, axis=1, keepdims=True) + EPS)
        result = (attended * scale * gain).astype(jnp.bfloat16)

        @pl.when(level != i)
        def _():
            oout[i] = result
            o_send(i).start()

        @pl.when(level == i)
        def _():
            headed[:, pl.ds(pl.multiple_of(level * HD, HD), HD)] = result

    wo_copy.wait()
    for h in range(heads):
        @pl.when(level != h)
        def _():
            here = headed.at[:, pl.ds(h * HD, HD)]
            pltpu.make_async_remote_copy(
                src_ref=here, dst_ref=here, send_sem=os_sem.at[0], recv_sem=or_sem.at[h],
                device_id={"frames": me}, device_id_type=MESH,
            ).wait_recv()

    cw = out_ref.shape[1]
    subs, sw = s1.shape[1], s1.shape[3]
    heads_in = headed[...]

    def partial_at(d, side, s):
        to = lax.rem(pair + d, pairs) * 2 + side
        cols = pl.ds(pl.multiple_of(to * cw + s * sw, sw), sw)
        return jnp.dot(heads_in, wo[:, cols], preferred_element_type=jnp.float32)

    def mate_send(d, s):
        return pltpu.make_async_remote_copy(
            src_ref=s1.at[d, s], dst_ref=r1.at[d, s],
            send_sem=s1_sem.at[d, s], recv_sem=r1_sem.at[d, s],
            device_id={"heads": mate}, device_id_type=MESH,
        )

    def pair_send(d, s):
        return pltpu.make_async_remote_copy(
            src_ref=s2.at[d - 1, s], dst_ref=r2.at[d - 1, s],
            send_sem=s2_sem.at[d - 1, s], recv_sem=r2_sem.at[d - 1, s],
            device_id={"heads": lax.rem(pair + d, pairs) * 2 + core}, device_id_type=MESH,
        )

    order = [(d % pairs, s) for d in range(1, pairs + 1) for s in range(subs)]
    for to in range(1, pairs + 1):
        d = to % pairs
        for s in range(subs):
            s1[d, s] = partial_at(d, 1 - core, s).astype(jnp.bfloat16)
            mate_send(d, s).start()
        for s in range(subs):
            own = partial_at(d, core, s)
            mate_send(d, s).wait_recv()
            own = own + r1[d, s].astype(jnp.float32)
            if d:
                s2[d - 1, s] = own.astype(jnp.bfloat16)
                pair_send(d, s).start()
            else:
                acc[s] = own
    for s in range(subs):
        whole = acc[s]
        for d in range(1, pairs):
            pair_send(d, s).wait_recv()
            whole = whole + r2[d - 1, s].astype(jnp.float32)
        out_ref[:, s * sw : (s + 1) * sw] = whole.astype(jnp.bfloat16)

    for d, s in order:
        mate_send(d, s).wait_send()
        if d:
            pair_send(d, s).wait_send()
    for i in range(heads):
        @pl.when(level != i)
        def _():
            o_send(i).wait_send()

        for d in range(1, group):
            forward(i * group + member, d).wait_send()
    for k in range(heads):
        @pl.when(head_at(k) != level)
        def _():
            kv_send(k, head_at(k) * group + member).wait_send()
            q_send(k, head_at(k) * group + member).wait_send()


def solution(mesh):
    n, nh = mesh.shape["frames"], mesh.shape["heads"]

    def per_device(tokens, norm_gain, w_query, w_key, w_value, head_gain, w_out):
        rows, depth = tokens.shape
        heads = w_query.shape[1] // HD
        width = w_out.shape[1]
        cw = width // nh
        subs = 1
        sw = cw // subs
        pairs = nh // 2
        group = n // heads
        per = 2 if heads % 2 == 0 else 1
        bf = jnp.bfloat16
        dma = pltpu.SemaphoreType.DMA
        hbm = pl.BlockSpec(memory_space=pltpu.HBM)
        vmem = pl.BlockSpec(memory_space=pltpu.VMEM)
        return pl.pallas_call(
            functools.partial(fused_kernel, n, nh),
            out_shape=jax.ShapeDtypeStruct((rows, cw), bf),
            in_specs=[hbm, vmem, hbm, hbm, hbm, vmem, hbm],
            out_specs=vmem,
            scratch_shapes=[
                pltpu.VMEM((rows, depth), bf),
                pltpu.VMEM((rows, depth), bf),
                pltpu.VMEM((heads, depth, 2 * HD), bf),
                pltpu.VMEM((heads // per, depth, per * HD), bf),
                pltpu.VMEM(w_out.shape, bf),
                pltpu.VMEM((heads, rows, 2 * HD), bf),
                pltpu.VMEM((heads, rows, HD), bf),
                pltpu.VMEM((n, rows, 2 * HD), bf),
                pltpu.VMEM((heads, rows, HD), bf),
                pltpu.VMEM((heads, rows, HD), bf),
                pltpu.VMEM((rows, heads * HD), bf),
                pltpu.VMEM((pairs, subs, rows, sw), bf),
                pltpu.VMEM((pairs, subs, rows, sw), bf),
                pltpu.VMEM((pairs - 1, subs, rows, sw), bf),
                pltpu.VMEM((pairs - 1, subs, rows, sw), bf),
                pltpu.VMEM((subs, rows, sw), jnp.float32),
                dma,
                dma((heads, 3)),
                dma,
                dma((heads,)),
                dma((heads,)),
                dma((heads, group)),
                dma((n,)),
                dma((heads,)),
                dma((heads,)),
                dma((heads,)),
                dma((pairs, subs)),
                dma((pairs, subs)),
                dma((pairs - 1, subs)),
                dma((pairs - 1, subs)),
            ],
            compiler_params=pltpu.CompilerParams(
                collective_id=0, has_side_effects=True, vmem_limit_bytes=55783424
            ),
            name="fused_block",
        )(tokens, norm_gain[None, :], w_query, w_key, w_value, head_gain[None, :], w_out)

    placed = (
        P("frames", None),
        P(),
        P(None, "heads"),
        P(None, "heads"),
        P(None, "heads"),
        P("heads"),
        P("heads", None),
    )
    return jax.shard_map(
        per_device, mesh=mesh, in_specs=placed, out_specs=P("frames", "heads"), check_vma=False
    )
```
